32 devices in a mesh: img: 2 (over y), sub: 4 (over z), rng: 4 (over x, core).
Axes of the slice: x: 2, y: 2, z: 4, core: 2. Of those that a mesh axis runs over, the one named last changes fastest.
Arguments:
- image: bfloat16 [2, 16, 128, 4096], P(None, ('img', 'sub'), None, 'rng'), parts along dimension 1, may hold values from -6 to 6
- interp_weights: bfloat16 [4, 2, 2, 2, 128, 128], replicated, may hold values from -0.25 to 0.25
- range_taps: float32 [4, 4], replicated, may hold values from -2 to 2
- range_shifts: int32 [4, 2, 128], replicated, may hold values from -8 to 5
Outputs:
- merged_image: bfloat16 [2, 16, 128, 4096], P(None, ('img', 'sub'), None, 'rng'), parts along dimension 1
The draws below stay inside these ranges and needn't reach their ends.
There are 2 independent parts, one for each index of `img`. The reference program is written for one: setup_inputs(seed, part) draws one part's arguments, and reference() takes and returns one part's arrays. A program takes and returns all parts, laid end to end along the dimension named above; an argument that names none is the same for every part. Nothing has to cross between parts.
All inputs are finite; a program needn't handle non-finite values.
Results may differ from the reference program's by a relative error of at most 0.0095.
Values may be sent and summed in bfloat16 or wider, within the bound.
A program may use at most 64 MiB of HBM per device.

```python
import math
import jax
import jax.numpy as jnp
import numpy as np

ANGLES = 128
RANGE = 4096
RIM = 8
TAPS = 4
LEVELS = 4
GROUPS = 2
SUBIMAGES = 8
N_SUB = 4


def touch_ends(entries, rng, smallest, top_value):
    spot = [jax.random.randint(jax.random.fold_in(rng, axis), (), 0, length) for axis, length in enumerate(entries.shape)]
    widest = entries.shape.index(max(entries.shape))
    next_to = spot[:widest] + [(spot[widest] + 1) % entries.shape[widest]] + spot[widest + 1:]
    return entries.at[tuple(spot)].set(smallest).at[tuple(next_to)].set(top_value)


def block_levels(own_key, dims, cuts, least, high):
    gain, own = 1.0, jax.random.fold_in(own_key, 6)
    for dim, shards_of in cuts:
        draws = jnp.exp(jax.random.uniform(jax.random.fold_in(own, dim), (shards_of,), jnp.float32, least / len(cuts), high / len(cuts)))
        gain = gain * jnp.repeat(draws, dims[dim] // shards_of).reshape([-1 if axis == dim else 1 for axis in range(len(dims))])
    return gain


def normal_values(stream_key, shape, deviation, bound, cuts=(), held_as=jnp.bfloat16):
    entries = deviation * jax.random.normal(stream_key, shape, jnp.float32)
    if cuts:
        entries = entries * block_levels(stream_key, shape, cuts, -0.22, 0.18)
    return jnp.clip(entries, -bound, bound).astype(held_as)


def setup_inputs(seed: int = 0, part: int = 0) -> dict:
    streams_of = jax.random.split(jax.random.key(seed), 5)
    part_keys = jax.random.split(jax.random.fold_in(streams_of[4], part), 5)
    image = normal_values(part_keys[0], (2, SUBIMAGES, ANGLES, RANGE), 1.0, 6.0, ((1, 4), (3, 4)))
    interp_weights = normal_values(streams_of[1], (LEVELS, 2, 2, 2, ANGLES, ANGLES), (4 * ANGLES) ** -0.5, 0.25)
    range_taps = normal_values(streams_of[2], (LEVELS, TAPS), 0.5, 2.0, (), jnp.float32)
    range_shifts = touch_ends(jax.random.randint(streams_of[3], (LEVELS, 2, ANGLES), 0 - RIM, RIM - TAPS + 2), jax.random.fold_in(streams_of[3], 1), 0 - RIM, (RIM - TAPS + 2) - 1).astype(jnp.int32)
    return dict(image=image, interp_weights=interp_weights, range_taps=range_taps, range_shifts=range_shifts)


phase_step = 2.0 * math.pi / 64.0


def rotate(merged_sum, level_index, half_index, range_start, range_width):
    angle_rows = half_index * ANGLES + jnp.arange(ANGLES, dtype=jnp.int32)
    range_cols = range_start + jnp.arange(range_width, dtype=jnp.int32)
    wrapped = (range_cols[None, :] * (angle_rows[:, None] + 1) * (7 + level_index)) % 64
    phase = wrapped.astype(jnp.float32) * phase_step
    cosine = jnp.cos(phase)
    sinus = jnp.sin(phase)
    return jnp.stack([merged_sum[0] * cosine - merged_sum[1] * sinus, merged_sum[0] * sinus + merged_sum[1] * cosine])


def reference(image, interp_weights, range_taps, range_shifts):
    bit_count = N_SUB.bit_length() - 1
    count = N_SUB * GROUPS
    current = image
    for level_index in range(LEVELS):
        bit = level_index % bit_count
        stride = 2 ** bit
        side_of_rows = (np.arange(count) // GROUPS // stride) % 2
        padded = jnp.pad(current, ((0, 0), (0, 0), (0, 0), (RIM, RIM)))
        shift_rows = range_shifts[level_index][side_of_rows]
        base_index = (RIM + shift_rows[:, :, None] + jnp.arange(RANGE, dtype=jnp.int32)[None, None, :]).astype(jnp.int32)
        total = jnp.zeros(current.shape, jnp.float32)
        for tap_index in range(TAPS):
            gathered = jnp.stack([jnp.take_along_axis(padded[channel], base_index + tap_index, axis=2) for channel in range(2)])
            total = total + range_taps[level_index, tap_index] * gathered.astype(jnp.float32)
        interpolated = total.astype(jnp.bfloat16)
        split_rows = interpolated.reshape(2, N_SUB // (2 * stride), 2, stride, GROUPS, ANGLES, RANGE)
        half_images = []
        for half_index in range(2):
            merged_sum = jnp.zeros((2, N_SUB // (2 * stride), stride, GROUPS, ANGLES, RANGE), jnp.float32)
            for side_index in range(2):
                weight_pair = interp_weights[level_index, side_index, half_index].astype(jnp.float32)
                block_matrix = jnp.stack([jnp.stack([weight_pair[0], -weight_pair[1]]), jnp.stack([weight_pair[1], weight_pair[0]])])
                source = split_rows[:, :, side_index].astype(jnp.float32)
                merged_sum = merged_sum + jnp.einsum('xcij,chmgjr->xhmgir', block_matrix, source)
            half_images.append(rotate(merged_sum, level_index, half_index, 0, RANGE))
        current = jnp.stack(half_images, axis=2).reshape(2, count, ANGLES, RANGE).astype(jnp.bfloat16)
    return current
```

```python
import math

import functools

import jax
import jax.numpy as jnp
import numpy as np
from jax import lax
from jax.experimental import pallas as pl
from jax.experimental.pallas import tpu as pltpu
from jax.sharding import PartitionSpec as P

ANGLES = 128
RANGE = 4096
RIM = 8
TAPS = 4
LEVELS = 4


phase_step = 2.0 * math.pi / 64.0


def padded_2(cells, sides, width):
    for axis, dim in sides:
        count = lax.axis_size(axis)
        ends = count - 1
        head = lax.slice_in_dim(cells, 0, width, axis=dim)
        tail = lax.slice_in_dim(cells, cells.shape[dim] - width, cells.shape[dim], axis=dim)
        cells = jnp.concatenate(
            [
                lax.ppermute(tail, axis, [(i, (i + 1) % count) for i in range(ends)]),
                cells,
                lax.ppermute(head, axis, [((i + 1) % count, i) for i in range(ends)]),
            ],
            axis=dim,
        )
    return cells


def from_partner(value, axis, stride):
    mask = 2**stride
    pairs = [(source, source ^ mask) for source in range(lax.axis_size(axis))]
    return lax.ppermute(value, axis, pairs)


def rotate(merged_sum, level_index, half_index, range_start, range_width):
    angle_rows = half_index * ANGLES + jnp.arange(ANGLES, dtype=jnp.int32)
    range_cols = range_start + jnp.arange(range_width, dtype=jnp.int32)
    wrapped = range_cols[None, :] * (angle_rows[:, None] + 1) * (7 + level_index) % 64
    phase = wrapped.astype(jnp.float32) * phase_step
    cosine = jnp.cos(phase)
    sinus = jnp.sin(phase)
    return jnp.stack(
        [
            merged_sum[0] * cosine - merged_sum[1] * sinus,
            merged_sum[0] * sinus + merged_sum[1] * cosine,
        ]
    )


def level_coef(range_taps, range_shifts, level_index, side_index):
    offsets = jnp.arange(2 * RIM + 1, dtype=jnp.int32) - RIM
    tap_ids = jnp.arange(TAPS, dtype=jnp.int32)
    hits = (
        range_shifts[level_index, side_index][:, None, None] + tap_ids[None, :, None]
        == offsets[None, None, :]
    )
    return jnp.einsum(
        "t,ato->ao",
        range_taps[level_index],
        hits.astype(jnp.float32),
        precision=lax.Precision.HIGHEST,
    )


def interpolate(padded, coef, range_width):
    total = None
    for offset_index in range(2 * RIM + 1):
        term = coef[:, offset_index, None] * padded[
            ..., offset_index : offset_index + range_width
        ].astype(jnp.float32)
        total = term if total is None else total + term
    return total.astype(jnp.bfloat16)


def block_of(weight_pair):
    return jnp.stack(
        [jnp.stack([weight_pair[0], -weight_pair[1]]), jnp.stack([weight_pair[1], weight_pair[0]])]
    )


def combine_sides(lower_rows, upper_rows, weights_level, half_index):
    chosen = lax.dynamic_index_in_dim(weights_level, half_index, 1, keepdims=False)
    merged_sum = None
    for side_index, source in ((0, lower_rows), (1, upper_rows)):
        product = jnp.einsum(
            "xcij,cgjr->xgir",
            block_of(chosen[side_index]),
            source,
            preferred_element_type=jnp.float32,
        )
        merged_sum = product if merged_sum is None else merged_sum + product
    return merged_sum


def on_device(image, interp_weights, range_taps, range_shifts):
    range_width = image.shape[3]
    sub_count = lax.axis_size("sub")
    bit_count = sub_count.bit_length() - 1
    sub_index = lax.axis_index("sub")
    range_start = lax.axis_index("rng") * range_width
    current = padded_2(image, (("rng", 3),), LEVELS * RIM)
    margin = LEVELS * RIM
    for level_index in range(LEVELS):
        bit = level_index % bit_count
        own_half = sub_index // 2**bit % 2
        padded = current
        margin = margin - RIM
        out_width = range_width + 2 * margin
        coef = jnp.where(
            own_half == 0,
            level_coef(range_taps, range_shifts, level_index, 0),
            level_coef(range_taps, range_shifts, level_index, 1),
        )
        own_rows = interpolate(padded, coef, out_width)
        partner = from_partner(own_rows, "sub", bit)
        lower_rows = jnp.where(own_half == 0, own_rows, partner)
        upper_rows = jnp.where(own_half == 0, partner, own_rows)
        merged = combine_sides(lower_rows, upper_rows, interp_weights[level_index], own_half)
        turned = rotate(merged, level_index, own_half, range_start - margin, out_width)
        global_cols = range_start - margin + jnp.arange(out_width, dtype=jnp.int32)
        inside = jnp.logical_and(global_cols >= 0, global_cols < RANGE)
        turned = jnp.where(inside, turned, 0.0)
        current = turned.astype(jnp.bfloat16)
    return current


PERIOD = 64
LANES = 128
HALO = LEVELS * RIM
MESH = pl.DeviceIdType.MESH
NT = (((1,), (1,)), ((), ()))


def phase_tables():
    a = np.arange(ANGLES)
    tables = np.zeros((LEVELS, 2, 2, PERIOD, ANGLES), np.float32)
    for level in range(LEVELS):
        for half in range(2):
            start = -HALO if level < LEVELS - 1 else 0
            r = (start + np.arange(PERIOD))[:, None]
            wrapped = (r * (half * ANGLES + a + 1)[None, :] * (7 + level)) % PERIOD
            phase = wrapped * phase_step
            tables[level, half, 0] = np.cos(phase)
            tables[level, half, 1] = np.sin(phase)
    last = np.swapaxes(tables[LEVELS - 1], -1, -2)
    last = np.concatenate([last] * (LANES // PERIOD), -1)
    return tables[: LEVELS - 1], last


def merge_kernel(
    n, rngs, image, weights, taps, shifts, rows_table, cols_table, out,
    xt, xin, big, table, xf, sh0, sh1, sh2, ybuf, stage,
    in_send, in_recv, left_send, left_recv, right_send, right_recv, out_send, out_recv,
):
    me = lax.axis_index("sub")
    place = lax.axis_index("rng")
    groups, width = image.shape[1], image.shape[3]
    block = width // n
    rows = block + 2 * HALO
    bits = n.bit_length() - 1

    def span(z):
        lo, hi = max(z * block - HALO, 0), min((z + 1) * block + HALO, width)
        return lo, lo - (z * block - HALO), hi - lo

    def in_copy(g, src, z):
        lo, off, size = span(z)
        return pltpu.make_async_remote_copy(
            src_ref=xt.at[g, :, pl.ds(lo, size), :],
            dst_ref=xin.at[g, src, :, pl.ds(off, size), :],
            send_sem=in_send.at[g, z],
            recv_sem=in_recv.at[g, src],
            device_id={"sub": z},
            device_id_type=MESH,
        )

    def left_copy(g, src):
        return pltpu.make_async_remote_copy(
            src_ref=xt.at[g, :, pl.ds(width - HALO, HALO), :],
            dst_ref=xin.at[g, src, :, pl.ds(0, HALO), :],
            send_sem=left_send.at[g],
            recv_sem=left_recv.at[g, src],
            device_id={"sub": 0, "rng": place + 1},
            device_id_type=MESH,
        )

    def right_copy(g, src):
        return pltpu.make_async_remote_copy(
            src_ref=xt.at[g, :, pl.ds(0, HALO), :],
            dst_ref=xin.at[g, src, :, pl.ds(rows - HALO, HALO), :],
            send_sem=right_send.at[g],
            recv_sem=right_recv.at[g, src],
            device_id={"sub": n - 1, "rng": place - 1},
            device_id_type=MESH,
        )

    def out_copy(g, z, owner):
        return pltpu.make_async_remote_copy(
            src_ref=stage.at[g, z],
            dst_ref=out.at[:, g, :, pl.ds(pl.multiple_of(owner * block, LANES), block)],
            send_sem=out_send.at[g, z],
            recv_sem=out_recv.at[g, owner],
            device_id={"sub": z},
            device_id_type=MESH,
        )

    eye = (
        lax.broadcasted_iota(jnp.int32, (LANES, LANES), 0)
        == lax.broadcasted_iota(jnp.int32, (LANES, LANES), 1)
    ).astype(jnp.bfloat16)

    for g in range(groups):
        for c in range(2):
            for k in range(width // LANES):
                cols = pl.ds(k * LANES, LANES)
                xt[g, c, cols, :] = lax.dot_general(
                    eye, image[c, g, :, cols], NT, preferred_element_type=jnp.float32
                ).astype(jnp.bfloat16)
        for z in range(n):

            @pl.when(me != z)
            def _():
                in_copy(g, me, z).start()

        @pl.when(place < rngs - 1)
        def _():
            left_copy(g, me).start()

        @pl.when(place > 0)
        def _():
            right_copy(g, me).start()

    at_left = jnp.logical_and(place == 0, me == 0)
    at_right = jnp.logical_and(place == rngs - 1, me == n - 1)

    for z in range(n):

        @pl.when(me == z)
        def _():
            lo, off, size = span(z)
            for g in range(groups):
                xin[g, z, :, off : off + size, :] = xt[g, :, lo : lo + size, :]

    @pl.when(at_left)
    def _():
        xin[:, :, :, :HALO, :] = jnp.zeros((groups, n, 2, HALO, ANGLES), jnp.bfloat16)

    @pl.when(at_right)
    def _():
        xin[:, :, :, rows - HALO :, :] = jnp.zeros((groups, n, 2, HALO, ANGLES), jnp.bfloat16)

    for level in range(LEVELS):
        for half in range(2):
            for side in range(2):
                real = weights[level, side, half, 0]
                imag = weights[level, side, half, 1]
                i = half * 2 * ANGLES
                j = side * 2 * ANGLES
                big[level, i : i + ANGLES, j : j + ANGLES] = real
                big[level, i : i + ANGLES, j + ANGLES : j + 2 * ANGLES] = -imag
                big[level, i + ANGLES : i + 2 * ANGLES, j : j + ANGLES] = imag
                big[level, i + ANGLES : i + 2 * ANGLES, j + ANGLES : j + 2 * ANGLES] = real
            if level < LEVELS - 1:
                for part in range(2):
                    for start in range(0, rows, PERIOD):
                        size = min(PERIOD, rows - start)
                        table[level, half, part, start : start + size, :] = rows_table[
                            level, half, part, :size, :
                        ]

    def per_group(g, carry):
        for z in range(n):

            @pl.when(me == z)
            def _():
                for src in range(n):
                    if src != z:
                        in_copy(g, src, z).wait_recv()

        @pl.when(jnp.logical_and(me == 0, place > 0))
        def _():
            for src in range(n):
                left_copy(g, src).wait_recv()

        @pl.when(jnp.logical_and(me == n - 1, place < rngs - 1))
        def _():
            for src in range(n):
                right_copy(g, src).wait_recv()

        for s in range(n):
            for c in range(2):
                xf[s, c, :rows, :] = xin[g, s, c].astype(jnp.float32)

        for level in range(LEVELS):
            mask = 2 ** (level % bits)
            base = RIM * level
            count = rows - 2 * base
            kept = count - 2 * RIM
            wide = kept + RIM

            def per_pair(pair, inner, level=level, mask=mask, base=base, count=count, kept=kept, wide=wide):
                low = pair // mask * (2 * mask) + pair % mask
                members = (low, low + mask)
                for side in range(2):
                    k = shifts[level, side][None, :] + RIM
                    on8, on4, on2, on1 = [(k // p) % 2 == 1 for p in (8, 4, 2, 1)]
                    for c in range(2):
                        s = members[side]
                        u = None
                        for t in range(TAPS):
                            term = taps[level, t] * xf[s, c, pl.ds(base + t, count), :]
                            u = term if u is None else u + term
                        v = jnp.where(on8, u[RIM:], u[:wide])
                        sh0[:wide] = v
                        v = jnp.where(on4, sh0[pl.ds(4, wide), :], v)
                        sh1[:wide] = v
                        v = jnp.where(on2, sh1[pl.ds(2, wide), :], v)
                        sh2[:wide] = v
                        v = jnp.where(on1, sh2[pl.ds(1, kept), :], v[:kept])
                        j = (side * 2 + c) * ANGLES
                        ybuf[:kept, j : j + ANGLES] = v.astype(jnp.bfloat16)
                y = ybuf[:kept, :]
                if level < LEVELS - 1:
                    z = lax.dot_general(y, big[level], NT, preferred_element_type=jnp.float32)
                    for half in range(2):
                        s = members[half]
                        j = half * 2 * ANGLES
                        re, im = z[:, j : j + ANGLES], z[:, j + ANGLES : j + 2 * ANGLES]
                        span_rows = pl.ds(base + RIM, kept)
                        cosine = table[level, half, 0, span_rows, :]
                        sinus = table[level, half, 1, span_rows, :]
                        xf[s, 0, span_rows, :] = re * cosine - im * sinus
                        xf[s, 1, span_rows, :] = re * sinus + im * cosine
                else:
                    z = lax.dot_general(big[level], y, NT, preferred_element_type=jnp.float32)
                    for half in range(2):
                        s = members[half]
                        i = half * 2 * ANGLES
                        cosine, sinus = cols_table[half, 0], cols_table[half, 1]
                        for start in range(0, block, LANES):
                            cols = slice(start, start + LANES)
                            re, im = z[i : i + ANGLES, cols], z[i + ANGLES : i + 2 * ANGLES, cols]
                            stage[g, s, 0, :, cols] = (re * cosine - im * sinus).astype(jnp.bfloat16)
                            stage[g, s, 1, :, cols] = (re * sinus + im * cosine).astype(jnp.bfloat16)
                return inner

            lax.fori_loop(0, n // 2, per_pair, 0)
            if level < LEVELS - 1:

                @pl.when(at_left)
                def _():
                    xf[:, :, :HALO, :] = jnp.zeros((n, 2, HALO, ANGLES), jnp.float32)

                @pl.when(at_right)
                def _():
                    xf[:, :, rows - HALO : rows, :] = jnp.zeros((n, 2, HALO, ANGLES), jnp.float32)

        for z in range(n):

            @pl.when(me != z)
            def _():
                out_copy(g, z, me).start()

            @pl.when(me == z)
            def _():
                out[:, g, :, z * block : (z + 1) * block] = stage[g, z]

        return carry

    lax.fori_loop(0, groups, per_group, 0)

    for g in range(groups):
        for z in range(n):

            @pl.when(me != z)
            def _():
                in_copy(g, me, z).wait_send()
                out_copy(g, z, me).wait_send()
                out_copy(g, z, z).wait_recv()

        @pl.when(place < rngs - 1)
        def _():
            left_copy(g, me).wait_send()

        @pl.when(place > 0)
        def _():
            right_copy(g, me).wait_send()


def in_one_kernel(n, rngs, image, interp_weights, range_taps, range_shifts):
    groups, width = image.shape[1], image.shape[3]
    block = width // n
    rows = block + 2 * HALO
    rows_table, cols_table = phase_tables()
    vmem = pl.BlockSpec(memory_space=pltpu.VMEM)
    dma = pltpu.SemaphoreType.DMA
    f32, bf16 = jnp.float32, jnp.bfloat16
    return pl.pallas_call(
        functools.partial(merge_kernel, n, rngs),
        out_shape=jax.ShapeDtypeStruct(image.shape, bf16),
        in_specs=[vmem, vmem, pl.BlockSpec(memory_space=pltpu.SMEM), vmem, vmem, vmem],
        out_specs=vmem,
        scratch_shapes=[
            pltpu.VMEM((groups, 2, width, ANGLES), bf16),
            pltpu.VMEM((groups, n, 2, rows, ANGLES), bf16),
            pltpu.VMEM((LEVELS, 4 * ANGLES, 4 * ANGLES), bf16),
            pltpu.VMEM((LEVELS - 1, 2, 2, rows, ANGLES), f32),
            pltpu.VMEM((n, 2, rows + 8, ANGLES), f32),
            pltpu.VMEM((rows + 8, ANGLES), f32),
            pltpu.VMEM((rows + 8, ANGLES), f32),
            pltpu.VMEM((rows + 8, ANGLES), f32),
            pltpu.VMEM((rows, 4 * ANGLES), bf16),
            pltpu.VMEM((groups, n, 2, ANGLES, block), bf16),
            dma((groups, n)),
            dma((groups, n)),
            dma((groups,)),
            dma((groups, n)),
            dma((groups,)),
            dma((groups, n)),
            dma((groups, n)),
            dma((groups, n)),
        ],
        compiler_params=pltpu.CompilerParams(has_side_effects=True),
    )(image, interp_weights, range_taps, range_shifts, rows_table, cols_table)


def fits_kernel(mesh, width):
    n = mesh.shape["sub"]
    block = width // n
    return n > 1 and n & (n - 1) == 0 and block % LANES == 0 and block >= HALO and ANGLES == LANES


def per_device(mesh, image, *rest):
    if fits_kernel(mesh, image.shape[3]):
        return in_one_kernel(mesh.shape["sub"], mesh.shape["rng"], image, *rest)
    return on_device(image, *rest)


def solution(mesh):
    return jax.shard_map(
        functools.partial(per_device, mesh),
        mesh=mesh,
        in_specs=(P(None, ("img", "sub"), None, "rng"), P(), P(), P()),
        out_specs=P(None, ("img", "sub"), None, "rng"),
        check_vma=False,
    )
```

```python
import math

import functools

import jax
import jax.numpy as jnp
import numpy as np
from jax import lax
from jax.experimental import pallas as pl
from jax.experimental.pallas import tpu as pltpu
from jax.sharding import PartitionSpec as P

ANGLES = 128
RANGE = 4096
RIM = 8
TAPS = 4
LEVELS = 4


phase_step = 2.0 * math.pi / 64.0


def padded_2(cells, sides, width):
    for axis, dim in sides:
        count = lax.axis_size(axis)
        ends = count - 1
        head = lax.slice_in_dim(cells, 0, width, axis=dim)
        tail = lax.slice_in_dim(cells, cells.shape[dim] - width, cells.shape[dim], axis=dim)
        cells = jnp.concatenate(
            [
                lax.ppermute(tail, axis, [(i, (i + 1) % count) for i in range(ends)]),
                cells,
                lax.ppermute(head, axis, [((i + 1) % count, i) for i in range(ends)]),
            ],
            axis=dim,
        )
    return cells


def from_partner(value, axis, stride):
    mask = 2**stride
    pairs = [(source, source ^ mask) for source in range(lax.axis_size(axis))]
    return lax.ppermute(value, axis, pairs)


def rotate(merged_sum, level_index, half_index, range_start, range_width):
    angle_rows = half_index * ANGLES + jnp.arange(ANGLES, dtype=jnp.int32)
    range_cols = range_start + jnp.arange(range_width, dtype=jnp.int32)
    wrapped = range_cols[None, :] * (angle_rows[:, None] + 1) * (7 + level_index) % 64
    phase = wrapped.astype(jnp.float32) * phase_step
    cosine = jnp.cos(phase)
    sinus = jnp.sin(phase)
    return jnp.stack(
        [
            merged_sum[0] * cosine - merged_sum[1] * sinus,
            merged_sum[0] * sinus + merged_sum[1] * cosine,
        ]
    )


def level_coef(range_taps, range_shifts, level_index, side_index):
    offsets = jnp.arange(2 * RIM + 1, dtype=jnp.int32) - RIM
    tap_ids = jnp.arange(TAPS, dtype=jnp.int32)
    hits = (
        range_shifts[level_index, side_index][:, None, None] + tap_ids[None, :, None]
        == offsets[None, None, :]
    )
    return jnp.einsum(
        "t,ato->ao",
        range_taps[level_index],
        hits.astype(jnp.float32),
        precision=lax.Precision.HIGHEST,
    )


def interpolate(padded, coef, range_width):
    total = None
    for offset_index in range(2 * RIM + 1):
        term = coef[:, offset_index, None] * padded[
            ..., offset_index : offset_index + range_width
        ].astype(jnp.float32)
        total = term if total is None else total + term
    return total.astype(jnp.bfloat16)


def block_of(weight_pair):
    return jnp.stack(
        [jnp.stack([weight_pair[0], -weight_pair[1]]), jnp.stack([weight_pair[1], weight_pair[0]])]
    )


def combine_sides(lower_rows, upper_rows, weights_level, half_index):
    chosen = lax.dynamic_index_in_dim(weights_level, half_index, 1, keepdims=False)
    merged_sum = None
    for side_index, source in ((0, lower_rows), (1, upper_rows)):
        product = jnp.einsum(
            "xcij,cgjr->xgir",
            block_of(chosen[side_index]),
            source,
            preferred_element_type=jnp.float32,
        )
        merged_sum = product if merged_sum is None else merged_sum + product
    return merged_sum


def on_device(image, interp_weights, range_taps, range_shifts):
    range_width = image.shape[3]
    sub_count = lax.axis_size("sub")
    bit_count = sub_count.bit_length() - 1
    sub_index = lax.axis_index("sub")
    range_start = lax.axis_index("rng") * range_width
    current = padded_2(image, (("rng", 3),), LEVELS * RIM)
    margin = LEVELS * RIM
    for level_index in range(LEVELS):
        bit = level_index % bit_count
        own_half = sub_index // 2**bit % 2
        padded = current
        margin = margin - RIM
        out_width = range_width + 2 * margin
        coef = jnp.where(
            own_half == 0,
            level_coef(range_taps, range_shifts, level_index, 0),
            level_coef(range_taps, range_shifts, level_index, 1),
        )
        own_rows = interpolate(padded, coef, out_width)
        partner = from_partner(own_rows, "sub", bit)
        lower_rows = jnp.where(own_half == 0, own_rows, partner)
        upper_rows = jnp.where(own_half == 0, partner, own_rows)
        merged = combine_sides(lower_rows, upper_rows, interp_weights[level_index], own_half)
        turned = rotate(merged, level_index, own_half, range_start - margin, out_width)
        global_cols = range_start - margin + jnp.arange(out_width, dtype=jnp.int32)
        inside = jnp.logical_and(global_cols >= 0, global_cols < RANGE)
        turned = jnp.where(inside, turned, 0.0)
        current = turned.astype(jnp.bfloat16)
    return current


PERIOD = 64
LANES = 128
HALO = LEVELS * RIM
MESH = pl.DeviceIdType.MESH
NT = (((1,), (1,)), ((), ()))


def phase_tables():
    a = np.arange(ANGLES)
    tables = np.zeros((LEVELS, 2, 2, PERIOD, ANGLES), np.float32)
    for level in range(LEVELS):
        for half in range(2):
            start = -HALO if level < LEVELS - 1 else 0
            r = (start + np.arange(PERIOD))[:, None]
            wrapped = (r * (half * ANGLES + a + 1)[None, :] * (7 + level)) % PERIOD
            phase = wrapped * phase_step
            tables[level, half, 0] = np.cos(phase)
            tables[level, half, 1] = np.sin(phase)
    last = np.swapaxes(tables[LEVELS - 1], -1, -2)
    last = np.concatenate([last] * (LANES // PERIOD), -1)
    return tables[: LEVELS - 1], last


def merge_kernel(
    n, rngs, image_hbm, weights_hbm, taps, shifts, rows_hbm, cols_hbm, out,
    image, weights, rows_table, cols_table, load_sem,
    xt, xin, big, table, xf, sh0, sh1, sh2, ybuf, stage,
    in_send, in_recv, left_send, left_recv, right_send, right_recv, twin_send, twin_recv, out_send, out_recv,
):
    me = lax.axis_index("sub")
    place = lax.axis_index("rng")
    groups, width = image_hbm.shape[1], image_hbm.shape[3]
    block = width // n
    rows = block + 2 * HALO
    bits = n.bit_length() - 1

    twin = place % 2
    first = place - twin
    mine = 2 * me + twin
    near = (HALO, 0), (0, HALO)

    def span(b):
        start = b % n * block
        lo = max(start - near[b % 2][0], 0)
        hi = min(start + block + near[b % 2][1], width)
        return lo, HALO + lo - start, hi - lo

    def in_copy(g, src, b):
        lo, off, size = span(b)
        return pltpu.make_async_remote_copy(
            src_ref=xt.at[g, :, pl.ds(lo, size), :],
            dst_ref=xin.at[g, src, :, pl.ds(off, size), :],
            send_sem=in_send.at[g, b],
            recv_sem=in_recv.at[g, src],
            device_id={"sub": b // 2, "rng": first + b % 2},
            device_id_type=MESH,
        )

    def twin_copy(g, size_from, size_to):
        return pltpu.make_async_remote_copy(
            src_ref=xin.at[g, :, :, pl.ds(size_from, HALO), :],
            dst_ref=xin.at[g, :, :, pl.ds(size_to, HALO), :],
            send_sem=twin_send.at[g],
            recv_sem=twin_recv.at[g],
            device_id={"rng": place + 1 - 2 * twin},
            device_id_type=MESH,
        )

    def left_copy(g, src):
        return pltpu.make_async_remote_copy(
            src_ref=xt.at[g, :, pl.ds(width - HALO, HALO), :],
            dst_ref=xin.at[g, src, :, pl.ds(0, HALO), :],
            send_sem=left_send.at[g],
            recv_sem=left_recv.at[g, src],
            device_id={"sub": (1 - twin) * (n // 2), "rng": first + 2 * twin},
            device_id_type=MESH,
        )

    def right_copy(g, src):
        return pltpu.make_async_remote_copy(
            src_ref=xt.at[g, :, pl.ds(0, HALO), :],
            dst_ref=xin.at[g, src, :, pl.ds(rows - HALO, HALO), :],
            send_sem=right_send.at[g],
            recv_sem=right_recv.at[g, src],
            device_id={"sub": twin * (n // 2) + (1 - twin) * n - 1, "rng": first - 1 + 2 * twin},
            device_id_type=MESH,
        )

    def out_copy(g, z, owner):
        return pltpu.make_async_remote_copy(
            src_ref=stage.at[g, z],
            dst_ref=out.at[:, g, :, pl.ds(pl.multiple_of(owner % n * block, LANES), block)],
            send_sem=out_send.at[g, z],
            recv_sem=out_recv.at[g, owner % n],
            device_id={"sub": z, "rng": first + owner // n},
            device_id_type=MESH,
        )

    left_self = jnp.logical_and(twin == 0, me == n // 2)
    left_out = jnp.logical_and(jnp.logical_not(left_self), place < rngs - 1)
    right_self = jnp.logical_and(twin == 1, me == n // 2 - 1)
    right_out = jnp.logical_and(jnp.logical_not(right_self), place > 0)

    head_from_left = jnp.logical_and(mine == 0, place > 0)
    tail_from_right = jnp.logical_and(mine == 2 * n - 1, place < rngs - 1)
    barrier = pltpu.get_barrier_semaphore()

    def ready(cond, z, r):
        @pl.when(cond)
        def _():
            pl.semaphore_signal(
                barrier, inc=1, device_id={"sub": z, "rng": r}, device_id_type=MESH
            )

    for z in range(n):
        for c in range(2):
            ready(mine != 2 * z + c, z, first + c)
        ready(head_from_left, z, place - 1)
        ready(tail_from_right, z, place + 1)

    loads = [
        pltpu.make_async_copy(image_hbm.at[:, g], image.at[:, g], load_sem.at[g])
        for g in range(groups)
    ]
    others = [
        pltpu.make_async_copy(src, dst, load_sem.at[groups + k])
        for k, (src, dst) in enumerate(
            ((weights_hbm, weights), (rows_hbm, rows_table), (cols_hbm, cols_table))
        )
    ]
    for copy in loads + others:
        copy.start()

    eye = (
        lax.broadcasted_iota(jnp.int32, (LANES, LANES), 0)
        == lax.broadcasted_iota(jnp.int32, (LANES, LANES), 1)
    ).astype(jnp.bfloat16)

    for g in range(groups):
        loads[g].wait()
        for c in range(2):
            for k in range(width // LANES):
                cols = pl.ds(k * LANES, LANES)
                xt[g, c, cols, :] = lax.dot_general(
                    eye, image[c, g, :, cols], NT, preferred_element_type=jnp.float32
                ).astype(jnp.bfloat16)
        if g == 0:
            sends_edge = jnp.where(twin == 1, place < rngs - 1, place > 0)
            pl.semaphore_wait(barrier, 2 * n - 1 + sends_edge.astype(jnp.int32))

        @pl.when(left_out)
        def _():
            left_copy(g, me).start()

        @pl.when(right_out)
        def _():
            right_copy(g, me).start()

        for b in range(2 * n):

            @pl.when(jnp.logical_and(twin == b // n, mine != b))
            def _():
                in_copy(g, me, b).start()

    at_left = jnp.logical_and(place == 0, me == 0)
    at_right = jnp.logical_and(place == rngs - 1, me == n - 1)

    for b in range(2 * n):
        z = b // 2
        if b % 2 == b // n:

            @pl.when(mine == b)
            def _():
                lo, off, size = span(b)
                for g in range(groups):
                    xin[g, z, :, off : off + size, :] = xt[g, :, lo : lo + size, :]

    @pl.when(left_self)
    def _():
        for g in range(groups):
            xin[g, n // 2, :, :HALO, :] = xt[g, :, width - HALO :, :]

    @pl.when(right_self)
    def _():
        for g in range(groups):
            xin[g, n // 2 - 1, :, rows - HALO :, :] = xt[g, :, :HALO, :]

    @pl.when(at_left)
    def _():
        xin[:, :, :, :HALO, :] = jnp.zeros((groups, n, 2, HALO, ANGLES), jnp.bfloat16)

    @pl.when(at_right)
    def _():
        xin[:, :, :, rows - HALO :, :] = jnp.zeros((groups, n, 2, HALO, ANGLES), jnp.bfloat16)

    for copy in others:
        copy.wait()

    for level in range(LEVELS):
        for half in range(2):
            for side in range(2):
                real = weights[level, side, half, 0]
                imag = weights[level, side, half, 1]
                i = half * 2 * ANGLES
                j = side * 2 * ANGLES
                big[level, i : i + ANGLES, j : j + ANGLES] = real
                big[level, i : i + ANGLES, j + ANGLES : j + 2 * ANGLES] = -imag
                big[level, i + ANGLES : i + 2 * ANGLES, j : j + ANGLES] = imag
                big[level, i + ANGLES : i + 2 * ANGLES, j + ANGLES : j + 2 * ANGLES] = real
            if level < LEVELS - 1:
                for part in range(2):
                    for start in range(0, rows, PERIOD):
                        size = min(PERIOD, rows - start)
                        table[level, half, part, start : start + size, :] = rows_table[
                            level, half, part, :size, :
                        ]

    def send_back(g, s):
        here = jnp.logical_and(s == me, twin == mine // n)

        @pl.when(jnp.logical_not(here))
        def _():
            out_copy(g, s, mine).start()

        @pl.when(here)
        def _():
            out[:, g, :, pl.ds(pl.multiple_of(mine % n * block, LANES), block)] = stage[g, s]

    def per_group(g, carry):
        for b in range(2 * n):

            @pl.when(mine == b)
            def _():
                for src in range(n):
                    if b % 2 != b // n or src != b // 2:
                        in_copy(g, src, b).wait_recv()
                if b % 2 == 0:
                    twin_copy(g, block, 0).start()
                else:
                    twin_copy(g, HALO, rows - HALO).start()

        @pl.when(jnp.logical_or(mine == n, jnp.logical_and(mine == 0, place > 0)))
        def _():
            for src in range(n):

                @pl.when(jnp.logical_or(mine == 0, src != n // 2))
                def _():
                    left_copy(g, src).wait_recv()

        @pl.when(jnp.logical_or(mine == n - 1, jnp.logical_and(mine == 2 * n - 1, place < rngs - 1)))
        def _():
            for src in range(n):

                @pl.when(jnp.logical_or(mine == 2 * n - 1, src != n // 2 - 1))
                def _():
                    right_copy(g, src).wait_recv()

        twin_copy(g, 0, 0).wait()

        for s in range(n):
            for c in range(2):
                xf[s, c, :rows, :] = xin[g, s, c].astype(jnp.float32)

        for level in range(LEVELS):
            mask = 2 ** (level % bits)
            base = RIM * level
            count = rows - 2 * base
            kept = count - 2 * RIM
            wide = kept + RIM

            def per_pair(pair, inner, level=level, mask=mask, base=base, count=count, kept=kept, wide=wide):
                low = pair // mask * (2 * mask) + pair % mask
                members = (low, low + mask)
                for side in range(2):
                    k = shifts[level, side][None, :] + RIM
                    on8, on4, on2, on1 = [(k // p) % 2 == 1 for p in (8, 4, 2, 1)]
                    for c in range(2):
                        s = members[side]
                        u = None
                        for t in range(TAPS):
                            term = taps[level, t] * xf[s, c, pl.ds(base + t, count), :]
                            u = term if u is None else u + term
                        v = jnp.where(on8, u[RIM:], u[:wide])
                        sh0[:wide] = v
                        v = jnp.where(on4, sh0[pl.ds(4, wide), :], v)
                        sh1[:wide] = v
                        v = jnp.where(on2, sh1[pl.ds(2, wide), :], v)
                        sh2[:wide] = v
                        v = jnp.where(on1, sh2[pl.ds(1, kept), :], v[:kept])
                        j = (side * 2 + c) * ANGLES
                        ybuf[:kept, j : j + ANGLES] = v.astype(jnp.bfloat16)
                y = ybuf[:kept, :]
                if level < LEVELS - 1:
                    z = lax.dot_general(y, big[level], NT, preferred_element_type=jnp.float32)
                    for half in range(2):
                        s = members[half]
                        j = half * 2 * ANGLES
                        re, im = z[:, j : j + ANGLES], z[:, j + ANGLES : j + 2 * ANGLES]
                        span_rows = pl.ds(base + RIM, kept)
                        cosine = table[level, half, 0, span_rows, :]
                        sinus = table[level, half, 1, span_rows, :]
                        xf[s, 0, span_rows, :] = re * cosine - im * sinus
                        xf[s, 1, span_rows, :] = re * sinus + im * cosine
                else:
                    z = lax.dot_general(big[level], y, NT, preferred_element_type=jnp.float32)
                    for half in range(2):
                        s = members[half]
                        i = half * 2 * ANGLES
                        cosine, sinus = cols_table[half, 0], cols_table[half, 1]
                        for start in range(0, block, LANES):
                            cols = slice(start, start + LANES)
                            re, im = z[i : i + ANGLES, cols], z[i + ANGLES : i + 2 * ANGLES, cols]
                            stage[g, s, 0, :, cols] = (re * cosine - im * sinus).astype(jnp.bfloat16)
                            stage[g, s, 1, :, cols] = (re * sinus + im * cosine).astype(jnp.bfloat16)
                    for half in range(2):
                        send_back(g, members[half])

                return inner

            lax.fori_loop(0, n // 2, per_pair, 0)
            if level < LEVELS - 1:

                @pl.when(at_left)
                def _():
                    xf[:, :, :HALO, :] = jnp.zeros((n, 2, HALO, ANGLES), jnp.float32)

                @pl.when(at_right)
                def _():
                    xf[:, :, rows - HALO : rows, :] = jnp.zeros((n, 2, HALO, ANGLES), jnp.float32)

        return carry

    lax.fori_loop(0, groups, per_group, 0)

    for g in range(groups):
        for b in range(2 * n):

            @pl.when(jnp.logical_and(twin == b // n, mine != b))
            def _():
                in_copy(g, me, b).wait_send()

        for z in range(n):

            @pl.when(jnp.logical_not(jnp.logical_and(me == z, twin == mine // n)))
            def _():
                out_copy(g, z, mine).wait_send()

            @pl.when(mine != n * twin + z)
            def _():
                out_copy(g, z, n * twin + z).wait_recv()

        @pl.when(left_out)
        def _():
            left_copy(g, me).wait_send()

        @pl.when(right_out)
        def _():
            right_copy(g, me).wait_send()


def in_one_kernel(n, rngs, image, interp_weights, range_taps, range_shifts):
    groups, width = image.shape[1], image.shape[3]
    block = width // n
    rows = block + 2 * HALO
    rows_table, cols_table = phase_tables()
    vmem = pl.BlockSpec(memory_space=pltpu.VMEM)
    hbm = pl.BlockSpec(memory_space=pl.ANY)
    dma = pltpu.SemaphoreType.DMA
    f32, bf16 = jnp.float32, jnp.bfloat16
    return pl.pallas_call(
        functools.partial(merge_kernel, n, rngs),
        out_shape=jax.ShapeDtypeStruct(image.shape, bf16),
        in_specs=[hbm, hbm, pl.BlockSpec(memory_space=pltpu.SMEM), vmem, hbm, hbm],
        out_specs=vmem,
        scratch_shapes=[
            pltpu.VMEM(image.shape, bf16),
            pltpu.VMEM(interp_weights.shape, bf16),
            pltpu.VMEM(rows_table.shape, f32),
            pltpu.VMEM(cols_table.shape, f32),
            dma((groups + 3,)),
            pltpu.VMEM((groups, 2, width, ANGLES), bf16),
            pltpu.VMEM((groups, n, 2, rows, ANGLES), bf16),
            pltpu.VMEM((LEVELS, 4 * ANGLES, 4 * ANGLES), bf16),
            pltpu.VMEM((LEVELS - 1, 2, 2, rows, ANGLES), f32),
            pltpu.VMEM((n, 2, rows + 8, ANGLES), f32),
            pltpu.VMEM((rows + 8, ANGLES), f32),
            pltpu.VMEM((rows + 8, ANGLES), f32),
            pltpu.VMEM((rows + 8, ANGLES), f32),
            pltpu.VMEM((rows, 4 * ANGLES), bf16),
            pltpu.VMEM((groups, n, 2, ANGLES, block), bf16),
            dma((groups, 2 * n)),
            dma((groups, n)),
            dma((groups,)),
            dma((groups, n)),
            dma((groups,)),
            dma((groups, n)),
            dma((groups,)),
            dma((groups,)),
            dma((groups, n)),
            dma((groups, n)),
        ],
        compiler_params=pltpu.CompilerParams(has_side_effects=True, collective_id=0),
    )(image, interp_weights, range_taps, range_shifts, rows_table, cols_table)


def fits_kernel(mesh, width):
    n = mesh.shape["sub"]
    block = width // n
    paired = mesh.shape["rng"] % 2 == 0
    return paired and n > 1 and n & (n - 1) == 0 and block % LANES == 0 and block >= HALO and ANGLES == LANES


def per_device(mesh, image, *rest):
    if fits_kernel(mesh, image.shape[3]):
        return in_one_kernel(mesh.shape["sub"], mesh.shape["rng"], image, *rest)
    return on_device(image, *rest)


def solution(mesh):
    return jax.shard_map(
        functools.partial(per_device, mesh),
        mesh=mesh,
        in_specs=(P(None, ("img", "sub"), None, "rng"), P(), P(), P()),
        out_specs=P(None, ("img", "sub"), None, "rng"),
        check_vma=False,
    )
```
